256 devices in a mesh: vert: 16 (over x, y), feat: 16 (over z, core).
Axes of the slice: x: 4, y: 4, z: 8, core: 2. Of those that a mesh axis runs over, the one named last changes fastest.
Arguments:
- features: bfloat16 [131072, 256], P('vert', 'feat'), may hold values from -6 to 6
- tiles: bfloat16 [1024, 16, 128, 128], P('vert'), may hold values from -0.1875 to 0.1875
- tile_cols: int32 [1024, 16], P('vert'), may hold values from 0 to 127
- tile_count: int32 [1024], P('vert'), may hold values from 1 to 16, as said below
- send_list: int32 [16, 16, 4], P('vert'), may hold values from 0 to 63
- weight: bfloat16 [256, 256], replicated, may hold values from -0.375 to 0.375
- bias: float32 [256], replicated, may hold values from -3 to 3
Outputs:
- node_out: bfloat16 [131072, 256], P(('vert', 'feat'))
The draws below stay inside these ranges and needn't reach their ends.
Inputs may be any that keep to these rules, and one draw needn't show every extreme that they name: Row block r uses tile places 0 to tile_count[r] - 1; in every draw some row block uses all 16.
All inputs are finite; a program needn't handle non-finite values.
Results may differ from the reference program's by a relative error of at most 0.0044.
Values may be sent and summed in bfloat16 or wider, within the bound.
A program may use at most 128 MiB of HBM per device.

```python
import jax
import jax.numpy as jnp
from jax import lax

F = 256
BLK = 128
K = 16
SLOTS = 4
RB_DEV = 64
NRB = 1024
NV = 131072
N_VERT = 16


def draw_tile_count(key, part):
    total = RB_DEV * N_VERT
    row_index = jnp.arange(total, dtype=jnp.int32)
    rank = row_index // RB_DEV
    ceiling = 1 + (K - 1) * (rank + 1) // N_VERT
    picks = jax.random.randint(key, (total,), 0, 1 << 20)
    counts = 1 + picks % ceiling
    chosen = jax.random.randint(jax.random.fold_in(key, 7), (), 0, total)
    return jnp.where(row_index == chosen, K, counts).astype(jnp.int32)


def with_ends(values, rng, least, top_value):
    spot = [jax.random.randint(jax.random.fold_in(rng, axis), (), 0, length) for axis, length in enumerate(values.shape)]
    longest = values.shape.index(max(values.shape))
    next_to = spot[:longest] + [(spot[longest] + 1) % values.shape[longest]] + spot[longest + 1:]
    return values.at[tuple(spot)].set(least).at[tuple(next_to)].set(top_value)


def block_levels(stream_key, dims, split, smallest, top_value):
    gain, own = 1.0, jax.random.fold_in(stream_key, 6)
    for dim, parts in split:
        steps = jnp.exp(jax.random.uniform(jax.random.fold_in(own, dim), (parts,), jnp.float32, smallest / len(split), top_value / len(split)))
        gain = gain * jnp.repeat(steps, dims[dim] // parts).reshape([-1 if axis == dim else 1 for axis in range(len(dims))])
    return gain


def scatter_about(rng, shape, width, reach, cuts=(), held_as=jnp.bfloat16):
    array = jax.random.normal(rng, shape, jnp.float32) * width
    if len(cuts) > 0:
        array = block_levels(rng, shape, cuts, -0.22, 0.18) * array
    return jnp.clip(array, min=-reach, max=reach).astype(held_as)


def setup_inputs(seed: int = 0) -> dict:
    streams_of = jax.random.split(jax.random.key(seed), 8)
    features = scatter_about(streams_of[0], (NV, F), 1.0, 6.0, ((0, 16), (1, 16)))
    tiles = scatter_about(streams_of[1], (NRB, K, BLK, BLK), (BLK * K // 2) ** -0.5, 0.1875, ((0, 16),))
    tile_cols = with_ends(jax.random.randint(streams_of[2], (NRB, K), 0, RB_DEV + N_VERT * SLOTS), jax.random.fold_in(streams_of[2], 1), 0, (RB_DEV + N_VERT * SLOTS) - 1).astype(jnp.int32)
    tile_count = draw_tile_count(jax.random.fold_in(streams_of[7], 71), 0)
    send_list = with_ends(jax.random.randint(streams_of[4], (N_VERT, N_VERT, SLOTS), 0, RB_DEV), jax.random.fold_in(streams_of[4], 1), 0, RB_DEV - 1).astype(jnp.int32)
    weight = scatter_about(streams_of[5], (F, F), F ** -0.5, 0.375)
    bias = scatter_about(streams_of[6], (F,), 0.5, 3.0, (), jnp.float32)
    return dict(features=features, tiles=tiles, tile_cols=tile_cols, tile_count=tile_count, send_list=send_list, weight=weight, bias=bias)


def reference(features, tiles, tile_cols, tile_count, send_list, weight, bias):
    row_owner = jnp.arange(RB_DEV * N_VERT, dtype=jnp.int32) // RB_DEV
    is_local = tile_cols < RB_DEV
    halo_slot = jnp.maximum(tile_cols - RB_DEV, 0)
    source = (halo_slot // SLOTS).astype(jnp.int32)
    position = (halo_slot % SLOTS).astype(jnp.int32)
    sent_block = send_list[source, row_owner[:, None], position]
    column = jnp.where(is_local, row_owner[:, None] * RB_DEV + tile_cols, source * RB_DEV + sent_block).astype(jnp.int32)
    blocks = features.reshape(RB_DEV * N_VERT, BLK, F)
    is_live = jnp.arange(K, dtype=jnp.int32)[None, :] < tile_count[:, None]

    def one_block(block_item):
        tile_row, col_row, live_row = block_item
        picked = blocks[col_row].astype(jnp.float32)
        products = jnp.einsum("kij,kjc->kic", tile_row.astype(jnp.float32), picked)
        kept = jnp.where(live_row[:, None, None], products, jnp.float32(0.0))
        return jnp.sum(kept, axis=0).astype(jnp.bfloat16)

    aggregated = lax.map(one_block, (tiles, column, is_live)).reshape(RB_DEV * N_VERT * BLK, F)
    mixed_rows = jnp.dot(aggregated, weight, preferred_element_type=jnp.float32) + bias
    return jnp.maximum(mixed_rows, jnp.float32(0.0)).astype(jnp.bfloat16)
```

```python
import jax
import jax.numpy as jnp
from jax import lax
from jax.experimental import pallas as pl
from jax.experimental.pallas import tpu as pltpu
from jax.sharding import PartitionSpec as P

MESH = pl.DeviceIdType.MESH
EDGE = 128
SIDE = 4
NT = (((1,), (1,)), ((), ()))
TN = (((0,), (0,)), ((), ()))


def farthest_first(length):
    return sorted(range(1, length), key=lambda d: (-min(d, length - d), d))


def plane_order(side):
    steps = [(a, b) for a in range(side) for b in range(side) if a or b]
    reach = lambda d: min(d, side - d)
    return sorted(steps, key=lambda ab: (-(reach(ab[0]) + reach(ab[1])), ab))


def kernel(
    x_hbm, tiles_hbm, cols, count, listed, w_ref, bias_ref, out_ref,
    x_own, own, ext, chosen, held, agg, recv,
    x_sem, tile_sem, near_sems, halo_send, halo_recv, fwd_send, fwd_recv, far_send, far_recv,
):
    slots, verts = listed.shape
    depth = cols.shape[0]
    blocks = cols.shape[1]
    chips = recv.shape[1]
    part = recv.shape[0]
    width = x_own.shape[0]
    v = lax.axis_index("vert")
    f = lax.axis_index("feat")
    core = f % 2
    chip = f // 2
    row, column = v // SIDE, v % SIDE
    sibling = chip * 2 + (1 - core)

    x_copy = pltpu.make_async_copy(x_hbm, x_own, x_sem)
    x_copy.start()

    vert_peers = []
    for a, b in plane_order(SIDE):
        vert_peers.append(((row + a) % SIDE) * SIDE + (column + b) % SIDE)
    feat_steps = farthest_first(chips)
    barrier = pltpu.get_barrier_semaphore()
    for peer in vert_peers:
        pl.semaphore_signal(barrier, inc=1, device_id=(peer, f), device_id_type=MESH)
    for d in feat_steps:
        other = ((chip + d) % chips) * 2 + core
        pl.semaphore_signal(barrier, inc=1, device_id=(v, other), device_id_type=MESH)
    pl.semaphore_signal(barrier, inc=1, device_id=(v, sibling), device_id_type=MESH)

    order = feat_steps + [0]
    tile_copies = []
    for d in order:
        first = ((chip + d) % chips) * 2 * part + core * part
        tile_copies.append(
            pltpu.make_async_copy(tiles_hbm.at[pl.ds(first, part)], held.at[d], tile_sem.at[d])
        )
    for copy in tile_copies:
        copy.start()

    x_copy.wait()
    mine = ext.at[core]
    for g in range(blocks):
        block = x_own[:, g * EDGE:(g + 1) * EDGE]
        own[g] = block
        mine[g] = block
    ext[0, blocks + verts * slots] = jnp.zeros((width, EDGE), ext.dtype)
    ext[1, blocks + verts * slots] = jnp.zeros((width, EDGE), ext.dtype)
    for u in range(verts):
        for s in range(slots):
            chosen[u, s] = own[listed[s, u]]
    for s in range(slots):
        mine[blocks + v * slots + s] = own[listed[s, v]]

    pl.semaphore_wait(barrier, len(vert_peers) + len(feat_steps) + 1)

    halo = []
    for j, peer in enumerate(vert_peers):
        copy = pltpu.make_async_remote_copy(
            src_ref=chosen.at[peer],
            dst_ref=ext.at[core, pl.ds(blocks + v * slots, slots)],
            send_sem=halo_send.at[j],
            recv_sem=halo_recv.at[j],
            device_id=(peer, f),
            device_id_type=MESH,
        )
        copy.start()
        halo.append(copy)
    near = pltpu.make_async_remote_copy(
        src_ref=ext.at[core, pl.ds(0, blocks)],
        dst_ref=ext.at[core, pl.ds(0, blocks)],
        send_sem=near_sems.at[0],
        recv_sem=near_sems.at[1],
        device_id=(v, sibling),
        device_id_type=MESH,
    )
    near.start()

    def forward(j, source):
        place = pl.ds(blocks + source * slots, slots)
        return pltpu.make_async_remote_copy(
            src_ref=ext.at[core, place],
            dst_ref=ext.at[core, place],
            send_sem=fwd_send.at[j],
            recv_sem=fwd_recv.at[j],
            device_id=(v, sibling),
            device_id_type=MESH,
        )

    fwd = [forward(len(vert_peers), v)]
    fwd[0].start()
    for j in reversed(range(len(vert_peers))):
        a, b = plane_order(SIDE)[j]
        source = ((row + SIDE - a) % SIDE) * SIDE + (column + SIDE - b) % SIDE
        halo[j].wait_recv()
        copy = forward(j, source)
        copy.start()
        fwd.append(copy)
    for copy in tile_copies:
        copy.wait()
    near.wait_recv()
    for copy in fwd:
        copy.wait_recv()

    def far(i, d):
        return pltpu.make_async_remote_copy(
            src_ref=agg.at[i, d],
            dst_ref=recv.at[i, chip],
            send_sem=far_send.at[i, d],
            recv_sem=far_recv.at[i, d],
            device_id=(v, ((chip + d) % chips) * 2 + core),
            device_id_type=MESH,
        )

    def quarter(i, carry):
        for d in order:
            r = ((chip + d) % chips) * 2 * part + core * part + i
            live = count[r]
            left = []
            for k in range(depth):
                at = jnp.where(k < live, cols[k, r], blocks + verts * slots)
                left.append(jnp.concatenate([ext[0, at], ext[1, at]], axis=0))
            right = [held[d, i, k] for k in range(depth)]
            total = lax.dot_general(
                jnp.concatenate(left, axis=1), jnp.concatenate(right, axis=1), NT,
                preferred_element_type=jnp.float32,
            )
            if d:
                agg[i, d] = total.astype(agg.dtype)
                far(i, d).start()
            else:
                recv[i, chip] = total.astype(recv.dtype)
        return carry

    lax.fori_loop(0, part, quarter, 0)

    def finish(i, carry):
        for d in feat_steps:
            far(i, d).wait_recv()
        hidden = recv[i].reshape(chips * recv.shape[2], EDGE)
        mixed = lax.dot_general(hidden, w_ref[...], TN, preferred_element_type=jnp.float32)
        place = pl.ds(pl.multiple_of(i * EDGE, EDGE), EDGE)
        out_ref[place, :] = jnp.maximum(mixed + bias_ref[...], 0.0).astype(out_ref.dtype)
        return carry

    lax.fori_loop(0, part, finish, 0)

    for copy in halo:
        copy.wait_send()
    near.wait_send()
    for copy in fwd:
        copy.wait_send()

    def drain(i, carry):
        for d in feat_steps:
            far(i, d).wait_send()
        return carry

    lax.fori_loop(0, part, drain, 0)


def per_device(features, tiles, tile_cols, tile_count, send_list, weight, bias):
    blocks, depth, edge, _ = tiles.shape
    width = features.shape[1]
    verts, slots = send_list.shape[1:]
    devices = lax.axis_size("feat")
    chips = devices // 2
    part = blocks // devices
    any_space = pl.BlockSpec(memory_space=pl.ANY)
    smem = pl.BlockSpec(memory_space=pltpu.SMEM)
    vmem = pl.BlockSpec(memory_space=pltpu.VMEM)
    dma = pltpu.SemaphoreType.DMA
    return pl.pallas_call(
        kernel,
        out_shape=jax.ShapeDtypeStruct((part * edge, weight.shape[1]), jnp.bfloat16),
        in_specs=[any_space, any_space, smem, smem, smem, vmem, vmem],
        out_specs=vmem,
        scratch_shapes=[
            pltpu.VMEM((width, blocks * edge), jnp.bfloat16),
            pltpu.VMEM((blocks, width, edge), jnp.bfloat16),
            pltpu.VMEM((2, blocks + verts * slots + 1, width, edge), jnp.bfloat16),
            pltpu.VMEM((verts, slots, width, edge), jnp.bfloat16),
            pltpu.VMEM((chips, part, depth, edge, edge), jnp.bfloat16),
            pltpu.VMEM((part, chips, 2 * width, edge), jnp.bfloat16),
            pltpu.VMEM((part, chips, 2 * width, edge), jnp.bfloat16),
            dma,
            dma((chips,)),
            dma((2,)),
            dma((verts - 1,)),
            dma((verts - 1,)),
            dma((verts,)),
            dma((verts,)),
            dma((part, chips)),
            dma((part, chips)),
        ],
        compiler_params=pltpu.CompilerParams(
            collective_id=0, has_side_effects=True, vmem_limit_bytes=60 * 1024 * 1024
        ),
    )(
        features.T, tiles, tile_cols.T, tile_count, send_list[0].T, weight, bias[None, :]
    )


def solution(mesh):
    return jax.shard_map(
        per_device,
        mesh=mesh,
        in_specs=(
            P("vert", "feat"),
            P("vert", None, None, None),
            P("vert", None),
            P("vert"),
            P("vert", None, None),
            P(),
            P(),
        ),
        out_specs=P(("vert", "feat"), None),
        check_vma=False,
    )
```

```python
import jax
import jax.numpy as jnp
from jax import lax
from jax.experimental import pallas as pl
from jax.experimental.pallas import tpu as pltpu
from jax.sharding import PartitionSpec as P

MESH = pl.DeviceIdType.MESH
EDGE = 128
SIDE = 4
NT = (((1,), (1,)), ((), ()))
TN = (((0,), (0,)), ((), ()))


def farthest_first(length):
    return sorted(range(1, length), key=lambda d: (-min(d, length - d), d))


def plane_order(side):
    steps = [(a, b) for a in range(side) for b in range(side) if a or b]
    reach = lambda d: min(d, side - d)
    return sorted(steps, key=lambda ab: (-(reach(ab[0]) + reach(ab[1])), ab))


def kernel(
    x_hbm, tiles_hbm, cols_hbm, count_hbm, listed_hbm, w_hbm, bias_hbm, out_ref,
    x_own, own, ext, chosen, held, agg, recv, cols, count, listed, w_ref, bias_ref,
    load_sems, tile_sem, known, near_sems, halo_send, halo_recv, fwd_send, fwd_recv, far_send, far_recv,
):
    slots, verts = listed.shape
    depth = cols.shape[0]
    blocks = cols.shape[1]
    chips = recv.shape[1]
    part = recv.shape[0]
    width = x_own.shape[0]
    v = lax.axis_index("vert")
    f = lax.axis_index("feat")
    core = f % 2
    chip = f // 2
    row, column = v // SIDE, v % SIDE
    sibling = chip * 2 + (1 - core)

    vert_peers = []
    for a, b in plane_order(SIDE):
        vert_peers.append(((row + a) % SIDE) * SIDE + (column + b) % SIDE)
    feat_steps = farthest_first(chips)
    barrier = pltpu.get_barrier_semaphore()
    for peer in vert_peers:
        pl.semaphore_signal(barrier, inc=1, device_id=(peer, chip * 2), device_id_type=MESH)
    for d in feat_steps:
        other = ((chip + d) % chips) * 2 + 1
        pl.semaphore_signal(barrier, inc=1, device_id=(v, other), device_id_type=MESH)

    @pl.when(core == 1)
    def _():
        pl.semaphore_signal(barrier, inc=1, device_id=(v, sibling), device_id_type=MESH)

    loads = []
    for j, (source, target) in enumerate((
        (x_hbm, x_own), (listed_hbm, listed), (cols_hbm, cols), (count_hbm, count), (w_hbm, w_ref), (bias_hbm, bias_ref),
    )):
        loads.append(pltpu.make_async_copy(source, target, load_sems.at[j]))
        loads[-1].start()

    order = feat_steps + [0]
    tile_copies = []
    for d in order:
        first = ((chip + d) % chips) * 2 * part + core * part
        tile_copies.append(
            pltpu.make_async_copy(tiles_hbm.at[pl.ds(first, part)], held.at[d], tile_sem.at[d])
        )
    for copy in tile_copies:
        copy.start()

    loads[0].wait()
    loads[1].wait()
    mine = ext.at[core]
    for g in range(blocks):
        block = x_own[:, g * EDGE:(g + 1) * EDGE]
        own[g] = block
        mine[g] = block
    ext[0, blocks + verts * slots] = jnp.zeros((width, EDGE), ext.dtype)
    ext[1, blocks + verts * slots] = jnp.zeros((width, EDGE), ext.dtype)
    for u in range(verts):
        for s in range(slots):
            chosen[u, s] = own[listed[s, u]]
    for s in range(slots):
        mine[blocks + v * slots + s] = own[listed[s, v]]

    @pl.when(core == 0)
    def _():
        pl.semaphore_wait(barrier, 2 * len(vert_peers) + 1)
        pl.semaphore_signal(known, inc=1, device_id=(v, sibling), device_id_type=MESH)

    @pl.when(core == 1)
    def _():
        pl.semaphore_wait(known, 1)

    halo = []
    for j, peer in enumerate(vert_peers):
        copy = pltpu.make_async_remote_copy(
            src_ref=chosen.at[peer],
            dst_ref=ext.at[core, pl.ds(blocks + v * slots, slots)],
            send_sem=halo_send.at[j],
            recv_sem=halo_recv.at[j],
            device_id=(peer, f),
            device_id_type=MESH,
        )
        copy.start()
        halo.append(copy)
    near = pltpu.make_async_remote_copy(
        src_ref=ext.at[core, pl.ds(0, blocks)],
        dst_ref=ext.at[core, pl.ds(0, blocks)],
        send_sem=near_sems.at[0],
        recv_sem=near_sems.at[1],
        device_id=(v, sibling),
        device_id_type=MESH,
    )
    near.start()

    def forward(j, source):
        place = pl.ds(blocks + source * slots, slots)
        return pltpu.make_async_remote_copy(
            src_ref=ext.at[core, place],
            dst_ref=ext.at[core, place],
            send_sem=fwd_send.at[j],
            recv_sem=fwd_recv.at[j],
            device_id=(v, sibling),
            device_id_type=MESH,
        )

    fwd = [forward(len(vert_peers), v)]
    fwd[0].start()
    for j in reversed(range(len(vert_peers))):
        a, b = plane_order(SIDE)[j]
        source = ((row + SIDE - a) % SIDE) * SIDE + (column + SIDE - b) % SIDE
        halo[j].wait_recv()
        copy = forward(j, source)
        copy.start()
        fwd.append(copy)

    @pl.when(core == 1)
    def _():
        pl.semaphore_wait(barrier, 2 * len(feat_steps))
        pl.semaphore_signal(known, inc=1, device_id=(v, sibling), device_id_type=MESH)

    @pl.when(core == 0)
    def _():
        pl.semaphore_wait(known, 1)

    for copy in loads[2:] + tile_copies:
        copy.wait()
    near.wait_recv()
    for copy in fwd:
        copy.wait_recv()

    def far(i, d):
        return pltpu.make_async_remote_copy(
            src_ref=agg.at[i, d],
            dst_ref=recv.at[i, chip],
            send_sem=far_send.at[i, d],
            recv_sem=far_recv.at[i, d],
            device_id=(v, ((chip + d) % chips) * 2 + core),
            device_id_type=MESH,
        )

    def quarter(i, carry):
        for d in order:
            r = ((chip + d) % chips) * 2 * part + core * part + i
            live = count[r]
            left = []
            for k in range(depth):
                at = jnp.where(k < live, cols[k, r], blocks + verts * slots)
                left.append(jnp.concatenate([ext[0, at], ext[1, at]], axis=0))
            right = [held[d, i, k] for k in range(depth)]
            total = lax.dot_general(
                jnp.concatenate(left, axis=1), jnp.concatenate(right, axis=1), NT,
                preferred_element_type=jnp.float32,
            )
            if d:
                agg[i, d] = total.astype(agg.dtype)
                far(i, d).start()
            else:
                recv[i, chip] = total.astype(recv.dtype)
        return carry

    lax.fori_loop(0, part, quarter, 0)

    def finish(i, carry):
        for d in feat_steps:
            far(i, d).wait_recv()
        hidden = recv[i].reshape(chips * recv.shape[2], EDGE)
        mixed = lax.dot_general(hidden, w_ref[...], TN, preferred_element_type=jnp.float32)
        place = pl.ds(pl.multiple_of(i * EDGE, EDGE), EDGE)
        out_ref[place, :] = jnp.maximum(mixed + bias_ref[...], 0.0).astype(out_ref.dtype)
        return carry

    lax.fori_loop(0, part, finish, 0)

    for copy in halo:
        copy.wait_send()
    near.wait_send()
    for copy in fwd:
        copy.wait_send()

    def drain(i, carry):
        for d in feat_steps:
            far(i, d).wait_send()
        return carry

    lax.fori_loop(0, part, drain, 0)


def per_device(features, tiles, tile_cols, tile_count, send_list, weight, bias):
    blocks, depth, edge, _ = tiles.shape
    width = features.shape[1]
    verts, slots = send_list.shape[1:]
    devices = lax.axis_size("feat")
    chips = devices // 2
    part = blocks // devices
    hbm = pl.BlockSpec(memory_space=pltpu.HBM)
    vmem = pl.BlockSpec(memory_space=pltpu.VMEM)
    dma = pltpu.SemaphoreType.DMA
    return pl.pallas_call(
        kernel,
        out_shape=jax.ShapeDtypeStruct((part * edge, weight.shape[1]), jnp.bfloat16),
        in_specs=[hbm] * 7,
        out_specs=vmem,
        scratch_shapes=[
            pltpu.VMEM((width, blocks * edge), jnp.bfloat16),
            pltpu.VMEM((blocks, width, edge), jnp.bfloat16),
            pltpu.VMEM((2, blocks + verts * slots + 1, width, edge), jnp.bfloat16),
            pltpu.VMEM((verts, slots, width, edge), jnp.bfloat16),
            pltpu.VMEM((chips, part, depth, edge, edge), jnp.bfloat16),
            pltpu.VMEM((part, chips, 2 * width, edge), jnp.bfloat16),
            pltpu.VMEM((part, chips, 2 * width, edge), jnp.bfloat16),
            pltpu.SMEM((depth, blocks), jnp.int32),
            pltpu.SMEM((blocks,), jnp.int32),
            pltpu.SMEM((slots, verts), jnp.int32),
            pltpu.VMEM(weight.shape, weight.dtype),
            pltpu.VMEM((1, weight.shape[1]), bias.dtype),
            dma((6,)),
            dma((chips,)),
            pltpu.SemaphoreType.REGULAR,
            dma((2,)),
            dma((verts - 1,)),
            dma((verts - 1,)),
            dma((verts,)),
            dma((verts,)),
            dma((part, chips)),
            dma((part, chips)),
        ],
        compiler_params=pltpu.CompilerParams(
            collective_id=0, has_side_effects=True, vmem_limit_bytes=28 * 1024 * 1024
        ),
    )(*(
        pltpu.with_memory_space_constraint(operand, pltpu.HBM)
        for operand in (features.T, tiles, tile_cols.T, tile_count, send_list[0].T, weight, bias[None, :])
    ))


def solution(mesh):
    return jax.shard_map(
        per_device,
        mesh=mesh,
        in_specs=(
            P("vert", "feat"),
            P("vert", None, None, None),
            P("vert", None),
            P("vert"),
            P("vert", None, None),
            P(),
            P(),
        ),
        out_specs=P(("vert", "feat"), None),
        check_vma=False,
    )
```

```python
import jax
import jax.numpy as jnp
from jax import lax
from jax.experimental import pallas as pl
from jax.experimental.pallas import tpu as pltpu
from jax.sharding import PartitionSpec as P

MESH = pl.DeviceIdType.MESH
EDGE = 128
SIDE = 4
TN = (((0,), (0,)), ((), ()))


def farthest_first(length):
    return sorted(range(1, length), key=lambda d: (-min(d, length - d), d))


def plane_order(side):
    steps = [(a, b) for a in range(side) for b in range(side) if a or b]
    reach = lambda d: min(d, side - d)
    return sorted(steps, key=lambda ab: (-(reach(ab[0]) + reach(ab[1])), ab))


def kernel(
    x_hbm, tiles_hbm, cols_hbm, count_hbm, listed_hbm, w_hbm, bias_hbm, out_ref,
    x_own, own, ext, chosen, held, agg, recv, cols, count, listed, w_ref, bias_ref,
    load_sems, tile_sem, known, near_sems, halo_send, halo_recv, fwd_send, fwd_recv, far_send, far_recv,
):
    slots, verts = listed.shape
    depth = cols.shape[0]
    blocks = cols.shape[1]
    chips, part = recv.shape[:2]
    width = x_own.shape[0]
    v = lax.axis_index("vert")
    f = lax.axis_index("feat")
    core = f % 2
    chip = f // 2
    row, column = v // SIDE, v % SIDE
    sibling = chip * 2 + (1 - core)

    vert_peers = []
    for a, b in plane_order(SIDE):
        vert_peers.append(((row + a) % SIDE) * SIDE + (column + b) % SIDE)
    feat_steps = farthest_first(chips)
    barrier = pltpu.get_barrier_semaphore()
    for peer in vert_peers:
        pl.semaphore_signal(barrier, inc=1, device_id=(peer, chip * 2), device_id_type=MESH)
    for d in feat_steps:
        other = ((chip + d) % chips) * 2 + 1
        pl.semaphore_signal(barrier, inc=1, device_id=(v, other), device_id_type=MESH)

    @pl.when(core == 1)
    def _():
        pl.semaphore_signal(barrier, inc=1, device_id=(v, sibling), device_id_type=MESH)

    loads = []
    for j, (source, target) in enumerate((
        (x_hbm, x_own), (listed_hbm, listed), (cols_hbm, cols), (count_hbm, count), (w_hbm, w_ref), (bias_hbm, bias_ref),
    )):
        loads.append(pltpu.make_async_copy(source, target, load_sems.at[j]))
        loads[-1].start()

    half = chips // 2
    tile_copies = []
    for t in range(half):
        for d in (half + t, half - 1 - t):
            first = ((chip + d) % chips) * 2 * part + core * part
            tile_copies.append((d, pltpu.make_async_copy(tiles_hbm.at[pl.ds(first, part)], held.at[d], tile_sem.at[d])))
    for _, copy in tile_copies:
        copy.start()

    loads[0].wait()
    loads[1].wait()
    mine = ext.at[core]
    for g in range(blocks):
        block = x_own[:, g * EDGE:(g + 1) * EDGE]
        own[g] = block
        mine[g] = block
    ext[0, blocks + verts * slots] = jnp.zeros((width, EDGE), ext.dtype)
    ext[1, blocks + verts * slots] = jnp.zeros((width, EDGE), ext.dtype)
    for u in range(verts):
        for s in range(slots):
            chosen[u, s] = own[listed[s, u]]
    for s in range(slots):
        mine[blocks + v * slots + s] = own[listed[s, v]]

    @pl.when(core == 0)
    def _():
        pl.semaphore_wait(barrier, 2 * len(vert_peers) + 1)
        pl.semaphore_signal(known, inc=1, device_id=(v, sibling), device_id_type=MESH)

    @pl.when(core == 1)
    def _():
        pl.semaphore_wait(known, 1)

    halo = []
    for j, peer in enumerate(vert_peers):
        copy = pltpu.make_async_remote_copy(
            src_ref=chosen.at[peer],
            dst_ref=ext.at[core, pl.ds(blocks + v * slots, slots)],
            send_sem=halo_send.at[j],
            recv_sem=halo_recv.at[j],
            device_id=(peer, f),
            device_id_type=MESH,
        )
        copy.start()
        halo.append(copy)
    near = pltpu.make_async_remote_copy(
        src_ref=ext.at[core, pl.ds(0, blocks)],
        dst_ref=ext.at[core, pl.ds(0, blocks)],
        send_sem=near_sems.at[0],
        recv_sem=near_sems.at[1],
        device_id=(v, sibling),
        device_id_type=MESH,
    )
    near.start()

    def forward(j, source):
        place = pl.ds(blocks + source * slots, slots)
        return pltpu.make_async_remote_copy(
            src_ref=ext.at[core, place],
            dst_ref=ext.at[core, place],
            send_sem=fwd_send.at[j],
            recv_sem=fwd_recv.at[j],
            device_id=(v, sibling),
            device_id_type=MESH,
        )

    def turn(i, carry):
        for k in range(depth):
            held[carry, i, k] = held[carry, i, k].T
        return carry

    for d, copy in tile_copies:
        copy.wait()
        lax.fori_loop(0, part, turn, d)

    fwd = [forward(len(vert_peers), v)]
    fwd[0].start()
    for j in reversed(range(len(vert_peers))):
        a, b = plane_order(SIDE)[j]
        source = ((row + SIDE - a) % SIDE) * SIDE + (column + SIDE - b) % SIDE
        halo[j].wait_recv()
        copy = forward(j, source)
        copy.start()
        fwd.append(copy)

    @pl.when(core == 1)
    def _():
        pl.semaphore_wait(barrier, 2 * len(feat_steps))
        pl.semaphore_signal(known, inc=1, device_id=(v, sibling), device_id_type=MESH)

    @pl.when(core == 0)
    def _():
        pl.semaphore_wait(known, 1)

    for copy in loads[2:]:
        copy.wait()
    near.wait_recv()
    for copy in fwd:
        copy.wait_recv()

    def far(d):
        return pltpu.make_async_remote_copy(
            src_ref=agg.at[d],
            dst_ref=recv.at[chip],
            send_sem=far_send.at[d],
            recv_sem=far_recv.at[d],
            device_id=(v, ((chip + d) % chips) * 2 + core),
            device_id_type=MESH,
        )

    def stage(t, carry):
        for d in (half + t, half - 1 - t):
            for i in range(part):
                r = ((chip + d) % chips) * 2 * part + core * part + i
                live = count[r]
                left = []
                for k in range(depth):
                    at = jnp.where(k < live, cols[k, r], blocks + verts * slots)
                    left.append(jnp.concatenate([ext[0, at], ext[1, at]], axis=0))
                total = jnp.dot(
                    jnp.concatenate(left, axis=1), held[d, i].reshape(depth * EDGE, EDGE),
                    preferred_element_type=jnp.float32,
                )
                agg[d, i] = total.astype(agg.dtype)
        far(half + t).start()

        @pl.when(t < half - 1)
        def _():
            far(half - 1 - t).start()

        return carry

    lax.fori_loop(0, half, stage, 0)
    recv[chip] = agg[0]
    for d in feat_steps:
        far(d).wait_recv()

    def finish(i, carry):
        hidden = recv[:, i].reshape(chips * recv.shape[2], EDGE)
        mixed = lax.dot_general(hidden, w_ref[...], TN, preferred_element_type=jnp.float32)
        place = pl.ds(pl.multiple_of(i * EDGE, EDGE), EDGE)
        out_ref[place, :] = jnp.maximum(mixed + bias_ref[...], 0.0).astype(out_ref.dtype)
        return carry

    lax.fori_loop(0, part, finish, 0)

    for copy in halo:
        copy.wait_send()
    near.wait_send()
    for copy in fwd:
        copy.wait_send()

    for d in feat_steps:
        far(d).wait_send()


def per_device(features, tiles, tile_cols, tile_count, send_list, weight, bias):
    blocks, depth, edge, _ = tiles.shape
    width = features.shape[1]
    verts, slots = send_list.shape[1:]
    devices = lax.axis_size("feat")
    chips = devices // 2
    part = blocks // devices
    hbm = pl.BlockSpec(memory_space=pltpu.HBM)
    vmem = pl.BlockSpec(memory_space=pltpu.VMEM)
    dma = pltpu.SemaphoreType.DMA
    return pl.pallas_call(
        kernel,
        out_shape=jax.ShapeDtypeStruct((part * edge, weight.shape[1]), jnp.bfloat16),
        in_specs=[hbm] * 7,
        out_specs=vmem,
        scratch_shapes=[
            pltpu.VMEM((width, blocks * edge), jnp.bfloat16),
            pltpu.VMEM((blocks, width, edge), jnp.bfloat16),
            pltpu.VMEM((2, blocks + verts * slots + 1, width, edge), jnp.bfloat16),
            pltpu.VMEM((verts, slots, width, edge), jnp.bfloat16),
            pltpu.VMEM((chips, part, depth, edge, edge), jnp.bfloat16),
            pltpu.VMEM((chips, part, 2 * width, edge), jnp.bfloat16),
            pltpu.VMEM((chips, part, 2 * width, edge), jnp.bfloat16),
            pltpu.SMEM((depth, blocks), jnp.int32),
            pltpu.SMEM((blocks,), jnp.int32),
            pltpu.SMEM((slots, verts), jnp.int32),
            pltpu.VMEM(weight.shape, weight.dtype),
            pltpu.VMEM((1, weight.shape[1]), bias.dtype),
            dma((6,)),
            dma((chips,)),
            pltpu.SemaphoreType.REGULAR,
            dma((2,)),
            dma((verts - 1,)),
            dma((verts - 1,)),
            dma((verts,)),
            dma((verts,)),
            dma((chips,)),
            dma((chips,)),
        ],
        compiler_params=pltpu.CompilerParams(
            collective_id=0, has_side_effects=True, vmem_limit_bytes=28 * 1024 * 1024
        ),
    )(*(
        pltpu.with_memory_space_constraint(operand, pltpu.HBM)
        for operand in (features.T, tiles, tile_cols.T, tile_count, send_list[0].T, weight, bias[None, :])
    ))


def solution(mesh):
    return jax.shard_map(
        per_device,
        mesh=mesh,
        in_specs=(
            P("vert", "feat"),
            P("vert", None, None, None),
            P("vert", None),
            P("vert"),
            P("vert", None, None),
            P(),
            P(),
        ),
        out_specs=P(("vert", "feat"), None),
        check_vma=False,
    )
```

```python
import jax
import jax.numpy as jnp
from jax import lax
from jax.experimental import pallas as pl
from jax.experimental.pallas import tpu as pltpu
from jax.sharding import PartitionSpec as P

MESH = pl.DeviceIdType.MESH
EDGE = 128
SIDE = 4
TN = (((0,), (0,)), ((), ()))


def farthest_first(length):
    return sorted(range(1, length), key=lambda d: (-min(d, length - d), d))


def hops(device):
    row, column = device // SIDE, device % SIDE
    return min(row, SIDE - row) + min(column, SIDE - column)


def plane_order(side):
    steps = [(a, b) for a in range(side) for b in range(side) if a or b]
    reach = lambda d: min(d, side - d)
    return sorted(steps, key=lambda ab: (-(reach(ab[0]) + reach(ab[1])), ab))


def kernel(
    x_hbm, tiles_hbm, cols_hbm, count_hbm, listed_hbm, w_hbm, bias_hbm, out_ref,
    x_own, own, ext, chosen, held, agg, recv, cols, count, listed, w_ref, bias_ref,
    load_sems, tile_sem, known, near_sems, halo_send, halo_recv, fwd_send, fwd_recv, far_send, far_recv,
):
    slots, verts = listed.shape
    depth = cols.shape[0]
    blocks = cols.shape[1]
    chips, part = recv.shape[:2]
    width = x_own.shape[0]
    v = lax.axis_index("vert")
    f = lax.axis_index("feat")
    core = f % 2
    chip = f // 2
    row, column = v // SIDE, v % SIDE
    cross = 1 - core
    sibling = chip * 2 + cross

    vert_order = sorted(range(verts), key=hops)
    barrier = pltpu.get_barrier_semaphore()
    for a, b in plane_order(SIDE):
        peer = ((row + a) % SIDE) * SIDE + (column + b) % SIDE
        pl.semaphore_signal(barrier, inc=1, device_id=(peer, chip * 2), device_id_type=MESH)
    for d in farthest_first(chips):
        other = ((chip + d) % chips) * 2 + 1
        pl.semaphore_signal(barrier, inc=1, device_id=(v, other), device_id_type=MESH)

    @pl.when(core == 1)
    def _():
        pl.semaphore_signal(barrier, inc=1, device_id=(v, sibling), device_id_type=MESH)

    loads = []
    for j, (source, target) in enumerate((
        (x_hbm, x_own), (listed_hbm, listed), (cols_hbm, cols), (count_hbm, count), (w_hbm, w_ref), (bias_hbm, bias_ref),
    )):
        loads.append(pltpu.make_async_copy(source, target, load_sems.at[j]))
        loads[-1].start()

    tile_copies = []
    for z in range(chips):
        first = z * 2 * part + core * part
        tile_copies.append((z, pltpu.make_async_copy(tiles_hbm.at[pl.ds(first, part)], held.at[z], tile_sem.at[z])))
    for _, copy in tile_copies:
        copy.start()

    loads[0].wait()
    loads[1].wait()
    mine = ext.at[core]
    for g in range(blocks):
        block = x_own[:, g * EDGE:(g + 1) * EDGE]
        own[g] = block
        mine[g] = block
    ext[0, blocks + verts * slots] = jnp.zeros((width, EDGE), ext.dtype)
    ext[1, blocks + verts * slots] = jnp.zeros((width, EDGE), ext.dtype)
    for u in range(verts):
        for s in range(slots):
            chosen[u, s] = own[listed[s, u]]
    for s in range(slots):
        mine[blocks + v * slots + s] = own[listed[s, v]]

    @pl.when(core == 0)
    def _():
        pl.semaphore_wait(barrier, 2 * (verts - 1) + 1)
        pl.semaphore_signal(known, inc=1, device_id=(v, sibling), device_id_type=MESH)

    @pl.when(core == 1)
    def _():
        pl.semaphore_wait(known, 1)

    def halo(peer):
        return pltpu.make_async_remote_copy(
            src_ref=chosen.at[peer],
            dst_ref=ext.at[core, pl.ds(blocks + v * slots, slots)],
            send_sem=halo_send.at[peer],
            recv_sem=halo_recv.at[v],
            device_id=(peer, sibling),
            device_id_type=MESH,
        )

    def arrived(source):
        place = ext.at[cross, pl.ds(blocks + source * slots, slots)]
        return pltpu.make_async_copy(place, place, halo_recv.at[source])

    for peer in vert_order:
        @pl.when(peer != v)
        def _():
            halo(peer).start()

    near = pltpu.make_async_remote_copy(
        src_ref=ext.at[core, pl.ds(0, blocks)],
        dst_ref=ext.at[core, pl.ds(0, blocks)],
        send_sem=near_sems.at[0],
        recv_sem=near_sems.at[1],
        device_id=(v, sibling),
        device_id_type=MESH,
    )
    near.start()

    def forward(source, side):
        place = pl.ds(blocks + source * slots, slots)
        return pltpu.make_async_remote_copy(
            src_ref=ext.at[side, place],
            dst_ref=ext.at[side, place],
            send_sem=fwd_send.at[source],
            recv_sem=fwd_recv.at[source],
            device_id=(v, sibling),
            device_id_type=MESH,
        )

    def turn(i, carry):
        for k in range(depth):
            held[carry, i, k] = held[carry, i, k].T
        return carry

    for d, copy in tile_copies:
        copy.wait()
        lax.fori_loop(0, part, turn, d)

    forward(v, core).start()
    for source in vert_order:
        @pl.when(source != v)
        def _():
            arrived(source).wait()
            forward(source, cross).start()

    @pl.when(core == 1)
    def _():
        pl.semaphore_wait(barrier, 2 * (chips - 1))
        pl.semaphore_signal(known, inc=1, device_id=(v, sibling), device_id_type=MESH)

    @pl.when(core == 0)
    def _():
        pl.semaphore_wait(known, 1)

    for copy in loads[2:]:
        copy.wait()
    near.wait_recv()
    for source in vert_order:
        forward(source, cross).wait_recv()

    def far(z, source):
        return pltpu.make_async_remote_copy(
            src_ref=agg.at[z],
            dst_ref=recv.at[source],
            send_sem=far_send.at[z],
            recv_sem=far_recv.at[source],
            device_id=(v, z * 2 + core),
            device_id_type=MESH,
        )

    def stage(destinations):
        for z in destinations:
            for i in range(part):
                r = z * 2 * part + core * part + i
                live = count[r]
                left = []
                for k in range(depth):
                    at = jnp.where(k < live, cols[k, r], blocks + verts * slots)
                    left.append(jnp.concatenate([ext[0, at], ext[1, at]], axis=0))
                total = jnp.dot(
                    jnp.concatenate(left, axis=1), held[z, i].reshape(depth * EDGE, EDGE),
                    preferred_element_type=jnp.float32,
                )
                agg[z, i] = total.astype(agg.dtype)
        for z in destinations:
            @pl.when(z != chip)
            def _():
                far(z, chip).start()

    def pair(t, carry):
        stage((2 * t + 1, 2 * t + 2))
        return carry

    stage((0,))
    lax.fori_loop(0, (chips - 2) // 2, pair, 0)
    stage((chips - 1,))
    recv[chip] = agg[chip]
    for source in reversed(range(chips)):
        @pl.when(source != chip)
        def _():
            far(source, source).wait_recv()

    for i in range(part):
        hidden = recv[:, i].reshape(chips * recv.shape[2], EDGE)
        mixed = lax.dot_general(hidden, w_ref[...], TN, preferred_element_type=jnp.float32)
        out_ref[i * EDGE:(i + 1) * EDGE, :] = jnp.maximum(mixed + bias_ref[...], 0.0).astype(out_ref.dtype)

    near.wait_send()
    for u in range(verts):
        @pl.when(u != v)
        def _():
            halo(u).wait_send()

        forward(u, cross).wait_send()
    for z in range(chips):
        @pl.when(z != chip)
        def _():
            far(z, chip).wait_send()


def per_device(features, tiles, tile_cols, tile_count, send_list, weight, bias):
    blocks, depth, edge, _ = tiles.shape
    width = features.shape[1]
    verts, slots = send_list.shape[1:]
    devices = lax.axis_size("feat")
    chips = devices // 2
    part = blocks // devices
    hbm = pl.BlockSpec(memory_space=pltpu.HBM)
    vmem = pl.BlockSpec(memory_space=pltpu.VMEM)
    dma = pltpu.SemaphoreType.DMA
    return pl.pallas_call(
        kernel,
        out_shape=jax.ShapeDtypeStruct((part * edge, weight.shape[1]), jnp.bfloat16),
        in_specs=[hbm] * 7,
        out_specs=vmem,
        scratch_shapes=[
            pltpu.VMEM((width, blocks * edge), jnp.bfloat16),
            pltpu.VMEM((blocks, width, edge), jnp.bfloat16),
            pltpu.VMEM((2, blocks + verts * slots + 1, width, edge), jnp.bfloat16),
            pltpu.VMEM((verts, slots, width, edge), jnp.bfloat16),
            pltpu.VMEM((chips, part, depth, edge, edge), jnp.bfloat16),
            pltpu.VMEM((chips, part, 2 * width, edge), jnp.bfloat16),
            pltpu.VMEM((chips, part, 2 * width, edge), jnp.bfloat16),
            pltpu.SMEM((depth, blocks), jnp.int32),
            pltpu.SMEM((blocks,), jnp.int32),
            pltpu.SMEM((slots, verts), jnp.int32),
            pltpu.VMEM(weight.shape, weight.dtype),
            pltpu.VMEM((1, weight.shape[1]), bias.dtype),
            dma((6,)),
            dma((chips,)),
            pltpu.SemaphoreType.REGULAR,
            dma((2,)),
            dma((verts,)),
            dma((verts,)),
            dma((verts,)),
            dma((verts,)),
            dma((chips,)),
            dma((chips,)),
        ],
        compiler_params=pltpu.CompilerParams(
            collective_id=0, has_side_effects=True, vmem_limit_bytes=28 * 1024 * 1024
        ),
    )(*(
        pltpu.with_memory_space_constraint(operand, pltpu.HBM)
        for operand in (features.T, tiles, tile_cols.T, tile_count, send_list[0].T, weight, bias[None, :])
    ))


def solution(mesh):
    return jax.shard_map(
        per_device,
        mesh=mesh,
        in_specs=(
            P("vert", "feat"),
            P("vert", None, None, None),
            P("vert", None),
            P("vert"),
            P("vert", None, None),
            P(),
            P(),
        ),
        out_specs=P(("vert", "feat"), None),
        check_vma=False,
    )
```

```python
import jax
import jax.numpy as jnp
from jax import lax
from jax.experimental import pallas as pl
from jax.experimental.pallas import tpu as pltpu
from jax.sharding import PartitionSpec as P

MESH = pl.DeviceIdType.MESH
EDGE = 128
SIDE = 4
TN = (((0,), (0,)), ((), ()))


def farthest_first(length):
    return sorted(range(1, length), key=lambda d: (-min(d, length - d), d))


def hops(device):
    row, column = device // SIDE, device % SIDE
    return min(row, SIDE - row) + min(column, SIDE - column)


def plane_order(side):
    steps = [(a, b) for a in range(side) for b in range(side) if a or b]
    reach = lambda d: min(d, side - d)
    return sorted(steps, key=lambda ab: (-(reach(ab[0]) + reach(ab[1])), ab))


def kernel(
    x_hbm, tiles_hbm, cols_hbm, count_hbm, listed_hbm, w_hbm, bias_hbm, out_ref,
    x_own, own, ext, chosen, held, agg, recv, cols, count, listed, w_ref, bias_ref,
    load_sems, tile_sem, near_sems, halo_send, halo_recv, fwd_send, fwd_recv, far_send, far_recv,
):
    slots, verts = listed.shape
    depth = cols.shape[0]
    blocks = cols.shape[1]
    chips, part = recv.shape[:2]
    width = x_own.shape[0]
    v = lax.axis_index("vert")
    f = lax.axis_index("feat")
    core = f % 2
    chip = f // 2
    row, column = v // SIDE, v % SIDE
    cross = 1 - core
    sibling = chip * 2 + cross

    vert_order = sorted(range(verts), key=hops)
    barrier = pltpu.get_barrier_semaphore()
    for a, b in plane_order(SIDE):
        peer = ((row + a) % SIDE) * SIDE + (column + b) % SIDE
        pl.semaphore_signal(barrier, inc=1, device_id=(peer, sibling), device_id_type=MESH)
    for d in farthest_first(chips):
        other = ((chip + d) % chips) * 2 + core
        pl.semaphore_signal(barrier, inc=1, device_id=(v, other), device_id_type=MESH)

    pl.semaphore_signal(barrier, inc=1, device_id=(v, sibling), device_id_type=MESH)

    loads = []
    for j, (source, target) in enumerate((
        (x_hbm, x_own), (listed_hbm, listed), (cols_hbm, cols), (count_hbm, count), (w_hbm, w_ref), (bias_hbm, bias_ref),
    )):
        loads.append(pltpu.make_async_copy(source, target, load_sems.at[j]))
        loads[-1].start()

    tile_copies = []
    for z in range(chips):
        first = z * 2 * part + core * part
        tile_copies.append((z, pltpu.make_async_copy(tiles_hbm.at[pl.ds(first, part)], held.at[z], tile_sem.at[z])))
    for _, copy in tile_copies:
        copy.start()

    loads[0].wait()
    loads[1].wait()
    mine = ext.at[core]
    for g in range(blocks):
        block = x_own[:, g * EDGE:(g + 1) * EDGE]
        own[g] = block
        mine[g] = block
    ext[0, blocks + verts * slots] = jnp.zeros((width, EDGE), ext.dtype)
    ext[1, blocks + verts * slots] = jnp.zeros((width, EDGE), ext.dtype)
    for u in range(verts):
        for s in range(slots):
            chosen[u, s] = own[listed[s, u]]
    for s in range(slots):
        mine[blocks + v * slots + s] = own[listed[s, v]]

    pl.semaphore_wait(barrier, verts + chips - 1)

    def halo(peer):
        return pltpu.make_async_remote_copy(
            src_ref=chosen.at[peer],
            dst_ref=ext.at[core, pl.ds(blocks + v * slots, slots)],
            send_sem=halo_send.at[peer],
            recv_sem=halo_recv.at[v],
            device_id=(peer, sibling),
            device_id_type=MESH,
        )

    def arrived(source):
        place = ext.at[cross, pl.ds(blocks + source * slots, slots)]
        return pltpu.make_async_copy(place, place, halo_recv.at[source])

    for a, b in plane_order(SIDE):
        halo(((row + a) % SIDE) * SIDE + (column + b) % SIDE).start()

    near = pltpu.make_async_remote_copy(
        src_ref=ext.at[core, pl.ds(0, blocks)],
        dst_ref=ext.at[core, pl.ds(0, blocks)],
        send_sem=near_sems.at[0],
        recv_sem=near_sems.at[1],
        device_id=(v, sibling),
        device_id_type=MESH,
    )
    near.start()

    def forward(source, side):
        place = pl.ds(blocks + source * slots, slots)
        return pltpu.make_async_remote_copy(
            src_ref=ext.at[side, place],
            dst_ref=ext.at[side, place],
            send_sem=fwd_send.at[source],
            recv_sem=fwd_recv.at[source],
            device_id=(v, sibling),
            device_id_type=MESH,
        )

    def turn(i, carry):
        for k in range(depth):
            held[carry, i, k] = held[carry, i, k].T
        return carry

    for d, copy in tile_copies:
        copy.wait()
        lax.fori_loop(0, part, turn, d)

    forward(v, core).start()
    for source in vert_order:
        @pl.when(source != v)
        def _():
            arrived(source).wait()
            forward(source, cross).start()

    for copy in loads[2:]:
        copy.wait()
    near.wait_recv()
    for source in vert_order:
        forward(source, cross).wait_recv()

    def far(z, source):
        return pltpu.make_async_remote_copy(
            src_ref=agg.at[z],
            dst_ref=recv.at[source],
            send_sem=far_send.at[z],
            recv_sem=far_recv.at[source],
            device_id=(v, z * 2 + core),
            device_id_type=MESH,
        )

    def stage(destinations):
        for z in destinations:
            for i in range(part):
                r = z * 2 * part + core * part + i
                live = count[r]
                left = []
                for k in range(depth):
                    at = jnp.where(k < live, cols[k, r], blocks + verts * slots)
                    left.append(jnp.concatenate([ext[0, at], ext[1, at]], axis=0))
                total = jnp.dot(
                    jnp.concatenate(left, axis=1), held[z, i].reshape(depth * EDGE, EDGE),
                    preferred_element_type=jnp.float32,
                )
                agg[z, i] = total.astype(agg.dtype)
        for z in destinations:
            @pl.when(z != chip)
            def _():
                far(z, chip).start()

    def pair(t, carry):
        stage((2 * t + half, 2 * t + half + 1))
        return carry

    half = chips // 2
    for z in range(half):
        stage((z,))
    lax.fori_loop(0, half // 2, pair, 0)
    recv[chip] = agg[chip]
    for source in reversed(range(chips)):
        @pl.when(source != chip)
        def _():
            far(source, source).wait_recv()

    for i in range(part):
        hidden = recv[:, i].reshape(chips * recv.shape[2], EDGE)
        mixed = lax.dot_general(hidden, w_ref[...], TN, preferred_element_type=jnp.float32)
        out_ref[i * EDGE:(i + 1) * EDGE, :] = jnp.maximum(mixed + bias_ref[...], 0.0).astype(out_ref.dtype)

    near.wait_send()
    for u in range(verts):
        @pl.when(u != v)
        def _():
            halo(u).wait_send()

        forward(u, cross).wait_send()
    for z in range(chips):
        @pl.when(z != chip)
        def _():
            far(z, chip).wait_send()


def per_device(features, tiles, tile_cols, tile_count, send_list, weight, bias):
    blocks, depth, edge, _ = tiles.shape
    width = features.shape[1]
    verts, slots = send_list.shape[1:]
    devices = lax.axis_size("feat")
    chips = devices // 2
    part = blocks // devices
    hbm = pl.BlockSpec(memory_space=pltpu.HBM)
    vmem = pl.BlockSpec(memory_space=pltpu.VMEM)
    dma = pltpu.SemaphoreType.DMA
    return pl.pallas_call(
        kernel,
        out_shape=jax.ShapeDtypeStruct((part * edge, weight.shape[1]), jnp.bfloat16),
        in_specs=[hbm] * 7,
        out_specs=vmem,
        scratch_shapes=[
            pltpu.VMEM((width, blocks * edge), jnp.bfloat16),
            pltpu.VMEM((blocks, width, edge), jnp.bfloat16),
            pltpu.VMEM((2, blocks + verts * slots + 1, width, edge), jnp.bfloat16),
            pltpu.VMEM((verts, slots, width, edge), jnp.bfloat16),
            pltpu.VMEM((chips, part, depth, edge, edge), jnp.bfloat16),
            pltpu.VMEM((chips, part, 2 * width, edge), jnp.bfloat16),
            pltpu.VMEM((chips, part, 2 * width, edge), jnp.bfloat16),
            pltpu.SMEM((depth, blocks), jnp.int32),
            pltpu.SMEM((blocks,), jnp.int32),
            pltpu.SMEM((slots, verts), jnp.int32),
            pltpu.VMEM(weight.shape, weight.dtype),
            pltpu.VMEM((1, weight.shape[1]), bias.dtype),
            dma((6,)),
            dma((chips,)),
            dma((2,)),
            dma((verts,)),
            dma((verts,)),
            dma((verts,)),
            dma((verts,)),
            dma((chips,)),
            dma((chips,)),
        ],
        compiler_params=pltpu.CompilerParams(
            collective_id=0, has_side_effects=True, vmem_limit_bytes=28 * 1024 * 1024
        ),
    )(*(
        pltpu.with_memory_space_constraint(operand, pltpu.HBM)
        for operand in (features.T, tiles, tile_cols.T, tile_count, send_list[0].T, weight, bias[None, :])
    ))


def solution(mesh):
    return jax.shard_map(
        per_device,
        mesh=mesh,
        in_specs=(
            P("vert", "feat"),
            P("vert", None, None, None),
            P("vert", None),
            P("vert"),
            P("vert", None, None),
            P(),
            P(),
        ),
        out_specs=P(("vert", "feat"), None),
        check_vma=False,
    )
```
